32 devices in a mesh: dp: 1 (over z), sp: 4 (over y), tp: 8 (over x, core).
Axes of the slice: x: 4, y: 4, z: 1, core: 2. Of those that a mesh axis runs over, the one named last changes fastest.
The devices are a block of a 4x4x8 slice.
Arguments:
- x_in: bfloat16 [32768, 4096], P(('dp', 'sp', 'tp'))
- seg_ids: int32 [32768], P(('dp', 'sp', 'tp'))
- w_zx: bfloat16 [4096, 2, 8192], P(None, None, 'tp')
- w_bc: bfloat16 [4096, 2, 1024], P(None, None, 'tp')
- w_dt: bfloat16 [4096, 128], P(None, 'tp')
- conv_x: bfloat16 [4, 8192], P(None, 'tp')
- conv_bc: bfloat16 [4, 2, 1024], P(None, None, 'tp')
- bias_x: bfloat16 [8192], P('tp')
- bias_bc: bfloat16 [2, 1024], P(None, 'tp')
- a_log: float32 [128], P('tp')
- dt_bias: float32 [128], P('tp')
- d_skip: float32 [128], P('tp')
- norm_w: bfloat16 [8192], P('tp')
- w_out: bfloat16 [8192, 4096], P('tp')
Outputs:
- output: bfloat16 [32768, 4096], P(('dp', 'sp', 'tp'))
All inputs are finite; a program needn't handle non-finite values.
Results may differ from the reference program's by a relative error of at most 0.00658122.
Values are sent between devices in bfloat16 or wider.
A program may use at most 768 MiB of HBM per device.

```python
import math
import jax
import jax.numpy as jnp
from jax import lax

D_MODEL = 4096
NUM_HEADS = 128
NUM_GROUPS = 8
TOK_DEV = 1024
SEQ_SHARDS = 4
HEAD_SHARDS = 8
HEAD_DIM = 64
STATE_DIM = 128
CONV_WIDTH = 4
SSD_TILE = 256
NORM_EPS = 1e-5
SEQ_LEN = TOK_DEV * SEQ_SHARDS * HEAD_SHARDS
BLOCK_LEN = TOK_DEV * HEAD_SHARDS
INNER_DIM = NUM_HEADS * HEAD_DIM
GROUP_WIDTH = NUM_GROUPS * STATE_DIM
PER_GROUP = NUM_HEADS // NUM_GROUPS


def setup_inputs(seed: int = 0, part: int = 0) -> dict:
    shared = jax.random.split(jax.random.key(seed), 12)
    part_key = jax.random.fold_in(jax.random.key(seed + 1), part)
    key_x, key_seg, key_pos = jax.random.split(part_key, 3)
    x_in = jax.random.normal(key_x, (SEQ_LEN, D_MODEL), jnp.float32)
    start_draw = jax.random.randint(key_seg, (SEQ_LEN,), 0, BLOCK_LEN)
    forced_pos = jax.random.randint(key_pos, (), 1, SEQ_LEN)
    is_start = (start_draw == 0) | (jnp.arange(SEQ_LEN) == forced_pos)
    seg_ids = jnp.cumsum(is_start.astype(jnp.int32)).astype(jnp.int32)
    in_scale = D_MODEL ** -0.5
    w_zx = jax.random.normal(shared[0], (D_MODEL, 2, INNER_DIM), jnp.float32) * in_scale
    w_bc = jax.random.normal(shared[1], (D_MODEL, 2, GROUP_WIDTH), jnp.float32) * in_scale
    w_dt = jax.random.normal(shared[2], (D_MODEL, NUM_HEADS), jnp.float32) * in_scale
    conv_x = jax.random.normal(shared[3], (CONV_WIDTH, INNER_DIM), jnp.float32) * 0.5
    conv_bc = jax.random.normal(shared[4], (CONV_WIDTH, 2, GROUP_WIDTH), jnp.float32) * 0.5
    bias_x = jax.random.normal(shared[5], (INNER_DIM,), jnp.float32) * 0.5
    bias_bc = jax.random.normal(shared[6], (2, GROUP_WIDTH), jnp.float32) * 0.5
    a_base = math.log(0.5 * math.sqrt(STATE_DIM / BLOCK_LEN))
    dt_base = math.log(1.0 / math.sqrt(BLOCK_LEN * STATE_DIM))
    a_log = a_base + jax.random.uniform(shared[7], (NUM_HEADS,), jnp.float32, -0.5, 0.5)
    dt_bias = dt_base + jax.random.uniform(shared[8], (NUM_HEADS,), jnp.float32, -0.5, 0.5)
    d_skip = jax.random.uniform(shared[9], (NUM_HEADS,), jnp.float32, 0.5, 1.5)
    norm_w = jax.random.uniform(shared[10], (INNER_DIM,), jnp.float32, 0.5, 1.5)
    w_out = jax.random.normal(shared[11], (INNER_DIM, D_MODEL), jnp.float32) * INNER_DIM ** -0.5
    return {'x_in': x_in.astype(jnp.bfloat16), 'seg_ids': seg_ids, 'w_zx': w_zx.astype(jnp.bfloat16), 'w_bc': w_bc.astype(jnp.bfloat16), 'w_dt': w_dt.astype(jnp.bfloat16), 'conv_x': conv_x.astype(jnp.bfloat16), 'conv_bc': conv_bc.astype(jnp.bfloat16), 'bias_x': bias_x.astype(jnp.bfloat16), 'bias_bc': bias_bc.astype(jnp.bfloat16), 'a_log': a_log, 'dt_bias': dt_bias, 'd_skip': d_skip, 'norm_w': norm_w.astype(jnp.bfloat16), 'w_out': w_out.astype(jnp.bfloat16)}


def reference(x_in, seg_ids, w_zx, w_bc, w_dt, conv_x, conv_bc, bias_x, bias_bc, a_log, dt_bias, d_skip, norm_w, w_out):
    halo_len = CONV_WIDTH - 1
    n_tiles = SEQ_LEN // SSD_TILE
    last_row = SSD_TILE - 1
    conv_w = jnp.concatenate([conv_x, conv_bc.reshape(CONV_WIDTH, 2 * GROUP_WIDTH)], axis=1).astype(jnp.float32)
    conv_b = jnp.concatenate([bias_x, bias_bc.reshape(2 * GROUP_WIDTH)]).astype(jnp.float32)
    decay_rate = jnp.exp(a_log).reshape(NUM_GROUPS, PER_GROUP)
    skip_gain = d_skip.reshape(NUM_GROUPS, PER_GROUP)
    w_zx_flat = w_zx.reshape(D_MODEL, 2 * INNER_DIM)
    w_bc_flat = w_bc.reshape(D_MODEL, 2 * GROUP_WIDTH)
    norm_gain = norm_w.astype(jnp.float32)
    causal = jnp.arange(SSD_TILE)[:, None] >= jnp.arange(SSD_TILE)[None, :]

    def step(carry, inputs):
        xbc_tail, seg_tail, state = carry
        x_tile, seg_tile = inputs
        zx_proj = jnp.dot(x_tile, w_zx_flat, preferred_element_type=jnp.float32).astype(jnp.bfloat16)
        bc_pre = jnp.dot(x_tile, w_bc_flat, preferred_element_type=jnp.float32).astype(jnp.bfloat16)
        dt_raw = jnp.dot(x_tile, w_dt, preferred_element_type=jnp.float32).astype(jnp.bfloat16)
        xbc = jnp.concatenate([zx_proj[:, INNER_DIM:], bc_pre], axis=1)
        padded = jnp.concatenate([xbc_tail, xbc], axis=0).astype(jnp.float32)
        seg_pad = jnp.concatenate([seg_tail, seg_tile])
        conv_acc = conv_b
        for tap_idx in range(CONV_WIDTH):
            keep_tap = (seg_pad[tap_idx:tap_idx + SSD_TILE] == seg_tile)[:, None]
            conv_acc = conv_acc + jnp.where(keep_tap, padded[tap_idx:tap_idx + SSD_TILE] * conv_w[tap_idx], 0.0)
        conv_act = jax.nn.silu(conv_acc).astype(jnp.bfloat16).astype(jnp.float32)
        x_ssm = conv_act[:, :INNER_DIM].reshape(SSD_TILE, NUM_GROUPS, PER_GROUP, HEAD_DIM)
        b_ssm = conv_act[:, INNER_DIM:INNER_DIM + GROUP_WIDTH].reshape(SSD_TILE, NUM_GROUPS, STATE_DIM)
        c_ssm = conv_act[:, INNER_DIM + GROUP_WIDTH:].reshape(SSD_TILE, NUM_GROUPS, STATE_DIM)
        dt_val = jax.nn.softplus(dt_raw.astype(jnp.float32) + dt_bias).reshape(SSD_TILE, NUM_GROUPS, PER_GROUP)
        log_a = -decay_rate * dt_val
        seg_prev = seg_tail[halo_len - 1]
        cum_log = jnp.cumsum(log_a, axis=0)
        same_doc = ((seg_tile[:, None] == seg_tile[None, :]) & causal)[:, :, None, None]
        decay = jnp.where(same_doc, jnp.exp(jnp.where(same_doc, cum_log[:, None] - cum_log[None, :], 0.0)), 0.0)
        scores = jnp.einsum('tgn,sgn->tsg', c_ssm, b_ssm)
        mix_mat = scores[..., None] * decay * dt_val[None]
        y_ssm = jnp.einsum('tsgr,sgrp->tgrp', mix_mat, x_ssm)
        keep_in = (seg_tile == seg_prev)[:, None, None]
        y_ssm = y_ssm + jnp.einsum('tgn,grpn->tgrp', c_ssm, state) * jnp.where(keep_in, jnp.exp(cum_log), 0.0)[..., None]
        y_ssm = y_ssm + skip_gain[None, :, :, None] * x_ssm
        keep_end = (seg_tile == seg_tile[last_row])[:, None, None]
        end_w = jnp.where(keep_end, jnp.exp(cum_log[last_row][None] - cum_log), 0.0) * dt_val
        carry_fac = jnp.where(seg_tile[last_row] == seg_prev, jnp.exp(cum_log[last_row]), 0.0)
        state = carry_fac[:, :, None, None] * state + jnp.einsum('sgrp,sgn->grpn', x_ssm * end_w[..., None], b_ssm)
        gate_val = jax.nn.silu(zx_proj[:, :INNER_DIM].astype(jnp.float32))
        gated = (y_ssm.reshape(SSD_TILE, INNER_DIM) * gate_val).reshape(SSD_TILE, NUM_GROUPS, INNER_DIM // NUM_GROUPS)
        normed = gated * lax.rsqrt(jnp.mean(gated * gated, axis=-1, keepdims=True) + NORM_EPS)
        y_norm = (normed.reshape(SSD_TILE, INNER_DIM) * norm_gain).astype(jnp.bfloat16)
        out_proj = jnp.dot(y_norm, w_out, preferred_element_type=jnp.float32)
        y_tile = (x_tile.astype(jnp.float32) + out_proj).astype(jnp.bfloat16)
        return (xbc[SSD_TILE - halo_len:], seg_tile[SSD_TILE - halo_len:], state), y_tile

    init_carry = (jnp.zeros((halo_len, INNER_DIM + 2 * GROUP_WIDTH), jnp.bfloat16), jnp.zeros((halo_len,), jnp.int32), jnp.zeros((NUM_GROUPS, PER_GROUP, HEAD_DIM, STATE_DIM), jnp.float32))
    tiles_in = (x_in.reshape(n_tiles, SSD_TILE, D_MODEL), seg_ids.reshape(n_tiles, SSD_TILE))
    scan_out = lax.scan(step, init_carry, tiles_in)
    return scan_out[1].reshape(SEQ_LEN, D_MODEL)
```

```python
import math, functools
import jax, jax.numpy as jnp
from jax import lax
from jax.sharding import PartitionSpec as P
from jax.experimental import pallas as pl
from jax.experimental.pallas import tpu as pltpu

F32, BF16 = jnp.float32, jnp.bfloat16
NEG = -1e30
LOG2E = 1.4426950408889634
CH = 128
NORM_EPS = 1e-5
CONV_WIDTH = 4
STATE_DIM = 128


def dotf(a, b):
    return jnp.dot(a, b, preferred_element_type=F32)


def split3_lanes(v, lane, heads):
    hi = v.astype(BF16).astype(F32)
    rest = v - hi
    mid = rest.astype(BF16).astype(F32)
    low = rest - mid
    part = jnp.where(lane < heads, hi, jnp.where(lane < 2 * heads, mid, jnp.where(lane < 3 * heads, low, 0.0)))
    return part.astype(BF16)


def ssd_kernel(xs_ref, bc_ref, dt_ref, comb_ref, row_ref, halo_ref, cw_ref, dtp_ref, dskip_ref, exp_ref,
               y_ref, c_ref, corr_ref, end_ref, dec_ref,
               state, prev, runcum, segp, *, heads, inner, ns):
    step = pl.program_id(0)
    rows = xs_ref.shape[0]
    n_sub = rows // CH
    hd = inner // heads
    width = inner + 2 * ns

    @pl.when(step == 0)
    def _():
        state[...] = jnp.zeros_like(state)
        runcum[...] = jnp.zeros_like(runcum)
        segp[...] = jnp.zeros_like(segp)
        prev[...] = jnp.zeros_like(prev)
        prev[CH - 8:, :] = halo_ref[...]

    it = lax.broadcasted_iota(jnp.int32, (CH, CH), 0)
    isx = lax.broadcasted_iota(jnp.int32, (CH, CH), 1)
    causal = it >= isx
    tri = jnp.where(causal, 1.0, 0.0).astype(BF16)
    tri3 = jnp.concatenate([tri, tri, tri], axis=1)
    half = lax.broadcasted_iota(jnp.int32, (CH, 2 * hd), 1) < hd
    for sub in range(n_sub):
        sl = pl.ds(sub * CH, CH)
        comb = comb_ref[sl, :]
        segb = comb >> 2
        dist = comb & 3
        shifts = []
        for j in (1, 2, 3):
            diag = isx - it
            keep = dist >= j
            in_cur = jnp.where((diag == -j) & keep, 1.0, 0.0)
            in_prev = jnp.where((diag == CH - j) & keep, 1.0, 0.0)
            shifts.append(jnp.concatenate([in_prev, in_cur], axis=1).astype(BF16))
        sh = jnp.concatenate(shifts, axis=0)

        def conv(cur, lo, hi):
            past = dotf(sh, jnp.concatenate([prev[:, lo:hi], cur], axis=0))
            acc = cur.astype(F32) * cw_ref[3:4, lo:hi] + cw_ref[4:5, lo:hi]
            for j in (1, 2, 3):
                acc = acc + past[(j - 1) * CH:j * CH] * cw_ref[3 - j:4 - j, lo:hi]
            prev[:, lo:hi] = cur
            return (acc + acc * jnp.tanh(acc)).astype(BF16)

        bc_act = conv(bc_ref[sl, :], inner, width)
        b_act = bc_act[:, :ns]
        c_act = bc_act[:, ns:]
        c_ref[sl, :] = c_act
        dt = dt_ref[sl, :].astype(F32) + dtp_ref[0:1, :]
        dt = jnp.maximum(dt, 0.0) + jnp.log1p(jnp.exp(-jnp.abs(dt)))
        la = dt * dtp_ref[1:2, :]
        hi3 = la.astype(BF16)
        r1 = la - hi3.astype(F32)
        mi3 = r1.astype(BF16)
        lo3 = (r1 - mi3.astype(F32)).astype(BF16)
        cum = dotf(tri3, jnp.concatenate([hi3, mi3, lo3], axis=0))
        l2dt = jnp.log2(dt)
        last = cum[CH - 1:CH, :]
        rt = (l2dt - cum).T
        seg_prev = segp[0:1, :]
        seg_last = segb[CH - 1:CH, :]
        mask = causal & (segb == row_ref[sub, :, :])
        scores = lax.dot_general(c_act, b_act, (((1,), (1,)), ((), ())), preferred_element_type=F32)
        wv = jnp.where(segb == seg_last, jnp.exp2(last - cum + l2dt), 0.0)
        fin = jnp.where(segb == seg_prev, jnp.exp2(cum), 0.0)
        carry = jnp.where(seg_last == seg_prev, jnp.exp2(last), 0.0)
        stack = jnp.concatenate([wv, fin, jnp.broadcast_to(carry, (8, CH))], axis=0)
        lane = lax.broadcasted_iota(jnp.int32, stack.shape, 1)
        stack = split3_lanes(stack, lane, heads)
        blk = 4 * hd
        for q in range(inner // blk):
            lo, hi = q * blk, (q + 1) * blk
            x_act = conv(xs_ref[sl, lo:hi], lo, hi)
            x_f = x_act.astype(F32)
            expd = dotf(stack, exp_ref[:, lo:hi])
            y_int = dotf(c_act, state[:, lo:hi].astype(BF16))
            y_base = y_int * expd[CH:2 * CH] + x_f * dskip_ref[0:1, lo:hi]
            xw = (x_f * expd[:CH]).astype(BF16)
            dstate = lax.dot_general(b_act, xw, (((0,), (0,)), ((), ())), preferred_element_type=F32)
            state[:, lo:hi] = state[:, lo:hi] * expd[2 * CH:2 * CH + 1] + dstate
            for p in range(2):
                mixes = []
                for h in (4 * q + 2 * p, 4 * q + 2 * p + 1):
                    arg = jnp.where(mask, cum[:, h:h + 1] + rt[h:h + 1, :], NEG)
                    mixes.append((scores * jnp.exp2(arg)).astype(BF16))
                lhs = jnp.concatenate(mixes, axis=1)
                xp = x_act[:, p * 2 * hd:(p + 1) * 2 * hd]
                zero = jnp.zeros_like(xp)
                rhs = jnp.concatenate([jnp.where(half, xp, zero), jnp.where(half, zero, xp)], axis=0)
                y_ref[sl, lo + p * 2 * hd:lo + (p + 1) * 2 * hd] = y_base[:, p * 2 * hd:(p + 1) * 2 * hd] + dotf(lhs, rhs)
        corr_ref[sl, :] = jnp.where(segb == 0, runcum[0:1, :] + cum, NEG)
        runcum[...] = runcum[...] + last
        segp[...] = jnp.broadcast_to(seg_last, segp.shape)

    @pl.when(step == pl.num_programs(0) - 1)
    def _():
        end_ref[...] = state[...]
        dec_ref[...] = jnp.where(segp[...] == 0, jnp.exp2(runcum[...]), 0.0)


def ssd_call(proj, comb, comb_row, halo, cw, dtp, dskip, expm, *, heads, inner, ns, rows=256):
    n_tok = proj.shape[0]
    width = inner + 2 * ns
    n_sub = rows // CH
    kern = functools.partial(ssd_kernel, heads=heads, inner=inner, ns=ns)
    full = lambda a: pl.BlockSpec(a.shape, lambda i: (0,) * a.ndim)
    return pl.pallas_call(
        kern,
        grid=(n_tok // rows,),
        in_specs=[
            pl.BlockSpec((rows, inner), lambda i: (i, 0)),
            pl.BlockSpec((rows, 2 * ns), lambda i: (i, inner // (2 * ns))),
            pl.BlockSpec((rows, CH), lambda i: (i, width // CH)),
            pl.BlockSpec((rows, CH), lambda i: (i, 0)),
            pl.BlockSpec((n_sub, 1, CH), lambda i: (i, 0, 0)),
            full(halo), full(cw), full(dtp), full(dskip), full(expm),
        ],
        out_specs=[
            pl.BlockSpec((rows, inner), lambda i: (i, 0)),
            pl.BlockSpec((rows, ns), lambda i: (i, 0)),
            pl.BlockSpec((rows, CH), lambda i: (i, 0)),
            pl.BlockSpec((ns, inner), lambda i: (0, 0)),
            pl.BlockSpec((8, CH), lambda i: (0, 0)),
        ],
        out_shape=[
            jax.ShapeDtypeStruct((n_tok, inner), F32),
            jax.ShapeDtypeStruct((n_tok, ns), BF16),
            jax.ShapeDtypeStruct((n_tok, CH), F32),
            jax.ShapeDtypeStruct((ns, inner), F32),
            jax.ShapeDtypeStruct((8, CH), F32),
        ],
        scratch_shapes=[
            pltpu.VMEM((ns, inner), F32),
            pltpu.VMEM((CH, width), BF16),
            pltpu.VMEM((8, CH), F32),
            pltpu.VMEM((8, CH), jnp.int32),
        ],
        compiler_params=pltpu.CompilerParams(dimension_semantics=("arbitrary",), vmem_limit_bytes=40 * 2**20),
        cost_estimate=pl.CostEstimate(flops=n_tok * 2 * 10**6, bytes_accessed=n_tok * 8000, transcendentals=0),
        name="ssd",
    )(proj, proj, proj, comb, comb_row, halo, cw, dtp, dskip, expm)


def gate_kernel(y_ref, c_ref, corr_ref, z_ref, st_ref, nw_ref, exp_ref, v_ref, *, heads, eps):
    rows = y_ref.shape[0]
    for sub in range(rows // CH):
        sl = pl.ds(sub * CH, CH)
        fac = jnp.exp2(corr_ref[sl, :])
        lane = lax.broadcasted_iota(jnp.int32, fac.shape, 1)
        fexp = dotf(split3_lanes(fac, lane, heads), exp_ref[...])
        y = y_ref[sl, :] + dotf(c_ref[sl, :], st_ref[...]) * fexp
        hz = z_ref[sl, :].astype(F32) * 0.5
        v = y * (hz + hz * jnp.tanh(hz))
        ms = jnp.mean(v * v, axis=-1, keepdims=True)
        v_ref[sl, :] = (v * lax.rsqrt(ms + eps) * nw_ref[0:1, :]).astype(BF16)


def gate_call(y, c, corr, z, st, nw, expm, *, heads, eps, rows=256):
    n_tok, inner = y.shape
    full = lambda a: pl.BlockSpec(a.shape, lambda i: (0,) * a.ndim)
    return pl.pallas_call(
        functools.partial(gate_kernel, heads=heads, eps=eps),
        grid=(n_tok // rows,),
        in_specs=[
            pl.BlockSpec((rows, inner), lambda i: (i, 0)),
            pl.BlockSpec((rows, c.shape[1]), lambda i: (i, 0)),
            pl.BlockSpec((rows, CH), lambda i: (i, 0)),
            pl.BlockSpec((rows, inner), lambda i: (i, 0)),
            full(st), full(nw), full(expm),
        ],
        out_specs=pl.BlockSpec((rows, inner), lambda i: (i, 0)),
        out_shape=jax.ShapeDtypeStruct((n_tok, inner), BF16),
        compiler_params=pltpu.CompilerParams(dimension_semantics=("arbitrary",), vmem_limit_bytes=40 * 2**20),
        cost_estimate=pl.CostEstimate(flops=n_tok * 10**6 // 2, bytes_accessed=n_tok * 8000, transcendentals=0),
        name="gate",
    )(y, c, corr, z, st, nw, expm)


def head_tables(heads, inner, a_log, dt_bias, d_skip):
    hd = inner // heads
    reps = CH // heads
    zeros = jnp.zeros((6, CH), F32)
    dtp = jnp.concatenate([jnp.tile(dt_bias, reps)[None], jnp.tile(-jnp.exp(a_log) * LOG2E, reps)[None], zeros], axis=0)
    dskip = jnp.repeat(d_skip, hd)[None]
    lane = jnp.arange(CH)[:, None]
    col_head = jnp.arange(inner)[None, :] // hd
    expm = ((lane < 3 * heads) & (lane % heads == col_head)).astype(BF16)
    return dtp, dskip, expm


def solution(mesh):
    seq_blocks = mesh.shape['sp']
    head_shards = mesh.shape['tp']
    token_spec = P(('dp', 'sp', 'tp'), None)
    seg_spec = P(('dp', 'sp', 'tp'))
    weight_specs = (P(None, None, 'tp'), P(None, None, 'tp'), P(None, 'tp'), P(None, 'tp'), P(None, None, 'tp'), P('tp'), P(None, 'tp'), P('tp'), P('tp'), P('tp'), P('tp'), P('tp', None))

    def body(x_loc, seg_loc, w_zx, w_bc, w_dt, conv_x, conv_bc, bias_x, bias_bc, a_log, dt_bias, d_skip, norm_w, w_out):
        d_model, _, inner = w_zx.shape
        heads = w_dt.shape[1]
        hd = inner // heads
        ns = STATE_DIM
        width = inner + 2 * ns
        sp = lax.axis_index('sp')
        x_blk = lax.all_gather(x_loc, 'tp', axis=0, tiled=True)
        n_tok = x_blk.shape[0]
        part = w_out.shape[0] // seq_blocks
        w_part = lax.dynamic_slice_in_dim(w_out, sp * part, part, axis=0)
        w_part, x_gate = lax.optimization_barrier((w_part, x_blk))
        w_all = lax.all_gather(w_part, ('tp', 'sp'), axis=0, tiled=True)
        seg_blk = lax.all_gather(seg_loc, 'tp', axis=0, tiled=True)
        to_next = [(s, s + 1) for s in range(seq_blocks - 1)]
        seg_tail = lax.ppermute(seg_blk[n_tok - 8:], 'sp', to_next)
        x_tail = lax.ppermute(x_gate[n_tok - 8:], 'sp', to_next)
        first = sp == 0
        seg_prev = jnp.where(first, seg_blk[0] - 1, seg_tail[7])
        segrel = seg_blk - seg_prev
        padded = jnp.concatenate([jnp.where(first, seg_blk[0] - 1, seg_tail[5:]), seg_blk])
        dist = sum((padded[3 - j:3 - j + n_tok] == seg_blk).astype(jnp.int32) for j in (1, 2, 3))
        comb = jnp.broadcast_to((segrel * 4 + dist)[:, None], (n_tok, CH))
        comb_row = segrel.reshape(n_tok // CH, 1, CH)
        w_bc2 = w_bc.reshape(d_model, 2 * ns)
        w_main = jnp.concatenate([w_zx[:, 1, :], w_bc2, jnp.tile(w_dt, (1, CH // heads))], axis=1)
        w_z = w_zx[:, 0, :]
        cw = jnp.concatenate([conv_x, conv_bc.reshape(CONV_WIDTH, 2 * ns)], axis=1).astype(F32)
        cb = jnp.concatenate([bias_x, bias_bc.reshape(2 * ns)])[None].astype(F32)
        cw = 0.5 * jnp.concatenate([cw, cb, jnp.zeros((3, width), F32)], axis=0)
        dtp, dskip, expm = head_tables(heads, inner, a_log, dt_bias, d_skip)
        halo = dotf(x_tail, w_main[:, :width]).astype(BF16)
        proj = dotf(x_gate, w_main).astype(BF16)
        y_loc, c_act, corr, end, dec = ssd_call(proj, comb, comb_row, halo, cw, dtp, dskip, expm, heads=heads, inner=inner, ns=ns)
        dec_row = jnp.repeat(dec[0:1, :heads], hd, axis=1)
        packed = jnp.concatenate([end, jnp.broadcast_to(dec_row, (8, inner))], axis=0)
        gathered = lax.all_gather(packed, 'sp', axis=0, tiled=False)
        x_z, _ = lax.optimization_barrier((x_gate, end))
        z = dotf(x_z, w_z).astype(BF16)
        st = jnp.zeros((ns, inner), F32)
        for src in range(seq_blocks - 1):
            nxt = gathered[src, ns:ns + 1] * st + gathered[src, :ns]
            st = jnp.where(src < sp, nxt, st)
        v = gate_call(y_loc, c_act, corr, z, st.astype(BF16), norm_w.astype(F32)[None], expm, heads=heads, eps=NORM_EPS)
        v_all = lax.all_to_all(v.reshape(head_shards, n_tok // head_shards, inner), 'tp', split_axis=0, concat_axis=0, tiled=False)
        out = jnp.einsum('stc,scd->td', v_all, w_all.reshape(head_shards, inner, d_model), preferred_element_type=F32)
        return (x_loc.astype(F32) + out).astype(BF16)

    return jax.shard_map(body, mesh=mesh, in_specs=(token_spec, seg_spec) + weight_specs, out_specs=token_spec, check_vma=False)
```

```python
import functools
import math
import jax
import jax.numpy as jnp
from jax import lax
from jax.sharding import PartitionSpec as P
from jax.experimental import pallas as pl
from jax.experimental.pallas import tpu as pltpu

F32, BF16 = jnp.float32, jnp.bfloat16
NEG = -1e30
LOG2E = 1.4426950408889634
CH = 128
NORM_EPS = 1e-5
CONV_WIDTH = 4
STATE_DIM = 128


def dotf(a, b):
    return jnp.dot(a, b, preferred_element_type=F32)


def split3_lanes(v, lane, heads):
    hi = v.astype(BF16).astype(F32)
    rest = v - hi
    mid = rest.astype(BF16).astype(F32)
    low = rest - mid
    part = jnp.where(lane < heads, hi, jnp.where(lane < 2 * heads, mid, jnp.where(lane < 3 * heads, low, 0.0)))
    return part.astype(BF16)


def ssd_kernel(*refs, heads, inner, ns, n_pieces, per):
    srcs = refs[:n_pieces]
    (comb_ref, row_ref, halo_ref, cw_ref, dtp_ref, dskip_ref, exp_ref,
     y_ref, c_ref, corr_ref, end_ref, dec_ref, buf, state, prev, runcum, segp, sems) = refs[n_pieces:]
    step = pl.program_id(0)
    rows = comb_ref.shape[0]
    slot = step & 1

    def fetch(t, where):
        for k in range(n_pieces):
            @pl.when(lax.div(t, per) == k)
            def _():
                pltpu.make_async_copy(srcs[k].at[pl.ds(lax.rem(t, per) * rows, rows), :], buf.at[where], sems.at[where]).start()

    @pl.when(step == 0)
    def _():
        fetch(0, 0)

    @pl.when(step + 1 < n_pieces * per)
    def _():
        fetch(step + 1, (step + 1) & 1)

    pltpu.make_async_copy(srcs[0].at[pl.ds(0, rows), :], buf.at[slot], sems.at[slot]).wait()
    n_sub = rows // CH
    hd = inner // heads
    width = inner + 2 * ns

    @pl.when(lax.rem(step, per) == 0)
    def _():
        state[...] = jnp.zeros_like(state)
        runcum[...] = jnp.zeros_like(runcum)
        segp[...] = jnp.zeros_like(segp)
        prev[...] = jnp.zeros_like(prev)
        prev[CH - 8:, :] = halo_ref[0]

    it = lax.broadcasted_iota(jnp.int32, (CH, CH), 0)
    isx = lax.broadcasted_iota(jnp.int32, (CH, CH), 1)
    causal = it >= isx
    tri = jnp.where(causal, 1.0, 0.0).astype(BF16)
    tri3 = jnp.concatenate([tri, tri, tri], axis=1)
    half = lax.broadcasted_iota(jnp.int32, (CH, 2 * hd), 1) < hd
    for sub in range(n_sub):
        sl = pl.ds(sub * CH, CH)
        comb = comb_ref[sl, :]
        segb = comb >> 2
        dist = comb & 3
        shifts = []
        for j in (1, 2, 3):
            diag = isx - it
            keep = dist >= j
            in_cur = jnp.where((diag == -j) & keep, 1.0, 0.0)
            in_prev = jnp.where((diag == CH - j) & keep, 1.0, 0.0)
            shifts.append(jnp.concatenate([in_prev, in_cur], axis=1).astype(BF16))
        sh = jnp.concatenate(shifts, axis=0)

        def conv(cur, lo, hi):
            past = dotf(sh, jnp.concatenate([prev[:, lo:hi], cur], axis=0))
            acc = cur.astype(F32) * cw_ref[3:4, lo:hi] + cw_ref[4:5, lo:hi]
            for j in (1, 2, 3):
                acc = acc + past[(j - 1) * CH:j * CH] * cw_ref[3 - j:4 - j, lo:hi]
            prev[:, lo:hi] = cur
            return (acc + acc * jnp.tanh(acc)).astype(BF16)

        bc_act = conv(buf[slot, sl, inner:width], inner, width)
        b_act = bc_act[:, :ns]
        c_act = bc_act[:, ns:]
        c_ref[sl, :] = c_act
        dt = buf[slot, sl, width:width + CH].astype(F32) + dtp_ref[0:1, :]
        dt = jnp.maximum(dt, 0.0) + jnp.log1p(jnp.exp(-jnp.abs(dt)))
        la = dt * dtp_ref[1:2, :]
        hi3 = la.astype(BF16)
        r1 = la - hi3.astype(F32)
        mi3 = r1.astype(BF16)
        lo3 = (r1 - mi3.astype(F32)).astype(BF16)
        cum = dotf(tri3, jnp.concatenate([hi3, mi3, lo3], axis=0))
        l2dt = jnp.log2(dt)
        last = cum[CH - 1:CH, :]
        rt = (l2dt - cum).T
        seg_prev = segp[0:1, :]
        seg_last = segb[CH - 1:CH, :]
        mask = causal & (segb == row_ref[sub, :, :])
        scores = lax.dot_general(c_act, b_act, (((1,), (1,)), ((), ())), preferred_element_type=F32)
        wv = jnp.where(segb == seg_last, jnp.exp2(last - cum + l2dt), 0.0)
        fin = jnp.where(segb == seg_prev, jnp.exp2(cum), 0.0)
        carry = jnp.where(seg_last == seg_prev, jnp.exp2(last), 0.0)
        stack = jnp.concatenate([wv, fin, jnp.broadcast_to(carry, (8, CH))], axis=0)
        lane = lax.broadcasted_iota(jnp.int32, stack.shape, 1)
        stack = split3_lanes(stack, lane, heads)
        blk = inner
        for q in range(inner // blk):
            lo, hi = q * blk, (q + 1) * blk
            x_act = conv(buf[slot, sl, lo:hi], lo, hi)
            x_f = x_act.astype(F32)
            expd = dotf(stack, exp_ref[:, lo:hi])
            y_int = dotf(c_act, state[:, lo:hi].astype(BF16))
            y_base = y_int * expd[CH:2 * CH] + x_f * dskip_ref[0:1, lo:hi]
            xw = (x_f * expd[:CH]).astype(BF16)
            dstate = lax.dot_general(b_act, xw, (((0,), (0,)), ((), ())), preferred_element_type=F32)
            state[:, lo:hi] = state[:, lo:hi] * expd[2 * CH:2 * CH + 1] + dstate
            for p in range(heads // 2):
                mixes = []
                for h in (2 * p, 2 * p + 1):
                    arg = jnp.where(mask, cum[:, h:h + 1] + rt[h:h + 1, :], NEG)
                    mixes.append((scores * jnp.exp2(arg)).astype(BF16))
                lhs = jnp.concatenate(mixes, axis=1)
                xp = x_act[:, p * 2 * hd:(p + 1) * 2 * hd]
                zero = jnp.zeros_like(xp)
                rhs = jnp.concatenate([jnp.where(half, xp, zero), jnp.where(half, zero, xp)], axis=0)
                y_ref[sl, lo + p * 2 * hd:lo + (p + 1) * 2 * hd] = y_base[:, p * 2 * hd:(p + 1) * 2 * hd] + dotf(lhs, rhs)
        corr_ref[sl, :] = jnp.where(segb == 0, runcum[0:1, :] + cum, NEG)
        runcum[...] = runcum[...] + last
        segp[...] = jnp.broadcast_to(seg_last, segp.shape)

    @pl.when(lax.rem(step, per) == per - 1)
    def _():
        end_ref[0] = state[...]
        dec_ref[0] = jnp.where(segp[...] == 0, jnp.exp2(runcum[...]), 0.0)


def ssd_call(pieces, comb, comb_row, halo, cw, dtp, dskip, expm, *, heads, inner, ns, rows):
    n_pieces = len(pieces)
    piece = pieces[0].shape[0]
    per = piece // rows
    n_tok = n_pieces * piece
    width = inner + 2 * ns
    n_sub = rows // CH
    kern = functools.partial(ssd_kernel, heads=heads, inner=inner, ns=ns, n_pieces=n_pieces, per=per)
    full = lambda a: pl.BlockSpec(a.shape, lambda i: (0,) * a.ndim)
    return pl.pallas_call(
        kern,
        grid=(n_pieces * per,),
        in_specs=[pl.BlockSpec(memory_space=pl.ANY)] * n_pieces + [
            pl.BlockSpec((rows, CH), lambda i: (i, 0)),
            pl.BlockSpec((n_sub, 1, CH), lambda i: (i, 0, 0)),
            pl.BlockSpec((1, 8, width), lambda i: (lax.div(i, per), 0, 0)),
            full(cw), full(dtp), full(dskip), full(expm),
        ],
        out_specs=[
            pl.BlockSpec((rows, inner), lambda i: (i, 0)),
            pl.BlockSpec((rows, ns), lambda i: (i, 0)),
            pl.BlockSpec((rows, CH), lambda i: (i, 0)),
            pl.BlockSpec((1, ns, inner), lambda i: (lax.div(i, per), 0, 0)),
            pl.BlockSpec((1, 8, CH), lambda i: (lax.div(i, per), 0, 0)),
        ],
        out_shape=[
            jax.ShapeDtypeStruct((n_tok, inner), F32),
            jax.ShapeDtypeStruct((n_tok, ns), BF16),
            jax.ShapeDtypeStruct((n_tok, CH), F32),
            jax.ShapeDtypeStruct((n_pieces, ns, inner), F32),
            jax.ShapeDtypeStruct((n_pieces, 8, CH), F32),
        ],
        scratch_shapes=[
            pltpu.VMEM((2, rows, width + CH), BF16),
            pltpu.VMEM((ns, inner), F32),
            pltpu.VMEM((CH, width), BF16),
            pltpu.VMEM((8, CH), F32),
            pltpu.VMEM((8, CH), jnp.int32),
            pltpu.SemaphoreType.DMA((2,)),
        ],
        compiler_params=pltpu.CompilerParams(dimension_semantics=("arbitrary",), vmem_limit_bytes=40 * 2**20),
        cost_estimate=pl.CostEstimate(flops=n_tok * 9 * 10**6, bytes_accessed=n_tok * 8000, transcendentals=0),
        name="ssd",
    )(*pieces, comb, comb_row, halo, cw, dtp, dskip, expm)


def gate_kernel(*refs, heads, eps, inner):
    sets = refs[:-2]
    exp_ref, v_ref = refs[-2], refs[-1]
    rows = v_ref.shape[0]
    for part in range(2):
        y_ref, c_ref, corr_ref, z_ref, st_ref, nw_ref = sets[6 * part:6 * part + 6]
        for sub in range(rows // CH):
            sl = pl.ds(sub * CH, CH)
            fac = jnp.exp2(corr_ref[sl, :])
            lane = lax.broadcasted_iota(jnp.int32, fac.shape, 1)
            fexp = dotf(split3_lanes(fac, lane, heads), exp_ref[...])
            y = y_ref[sl, :] + dotf(c_ref[sl, :], st_ref[...]) * fexp
            hz = z_ref[sl, :].astype(F32) * 0.5
            v = y * (hz + hz * jnp.tanh(hz))
            ms = jnp.mean(v * v, axis=-1, keepdims=True)
            v_ref[sl, part * inner:(part + 1) * inner] = (v * lax.rsqrt(ms + eps) * nw_ref[0:1, :]).astype(BF16)


def gate_call(sets, expm, where, piece, *, heads, eps, rows=256):
    inner = sets[0][0].shape[1]
    off = where * (piece // rows)
    full = lambda a: pl.BlockSpec(a.shape, lambda i: (0,) * a.ndim)
    specs, args = [], []
    for y, c, corr, z, st, nw in sets:
        specs += [pl.BlockSpec((rows, inner), lambda i: (i + off, 0)), pl.BlockSpec((rows, c.shape[1]), lambda i: (i + off, 0)),
                  pl.BlockSpec((rows, CH), lambda i: (i + off, 0)), pl.BlockSpec((rows, inner), lambda i: (i, 0)), full(st), full(nw)]
        args += [y, c, corr, z, st, nw]
    return pl.pallas_call(
        functools.partial(gate_kernel, heads=heads, eps=eps, inner=inner),
        grid=(piece // rows,),
        in_specs=specs + [full(expm)],
        out_specs=pl.BlockSpec((rows, 2 * inner), lambda i: (i, 0)),
        out_shape=jax.ShapeDtypeStruct((piece, 2 * inner), BF16),
        compiler_params=pltpu.CompilerParams(dimension_semantics=("arbitrary",), vmem_limit_bytes=40 * 2**20),
        cost_estimate=pl.CostEstimate(flops=piece * 6 * 10**6, bytes_accessed=piece * 16000, transcendentals=0),
        name="gate",
    )(*args, expm)


def out_kernel(idx_ref, va_ref, vb_ref, w_ref, *rest, last):
    del idx_ref
    j = pl.program_id(1)
    half = pl.num_programs(1) // 2
    if last:
        x_ref, before_ref, o_ref, acc = rest
    else:
        acc, = rest

    @pl.when(j == 0)
    def _():
        acc[...] = before_ref[...] if last else jnp.zeros_like(acc)

    v = jnp.where(j < half, va_ref[...], vb_ref[...])
    acc[...] += dotf(v, w_ref[...])
    if last:
        @pl.when(j == 2 * half - 1)
        def _():
            o_ref[...] = (x_ref[...].astype(F32) + acc[...]).astype(BF16)


def out_call(idx, va, vb, w_all, inner, extra):
    piece = va.shape[0]
    d_model = w_all.shape[1]
    cols = math.gcd(d_model, 1024)
    last = extra is not None
    specs = [
        pl.BlockSpec((piece, inner), lambda n, j, idx: (0, jnp.minimum(j, 1))),
        pl.BlockSpec((piece, inner), lambda n, j, idx: (0, jnp.maximum(j - 2, 0))),
        pl.BlockSpec((inner, cols), lambda n, j, idx: (idx[j], n)),
    ]
    tile = pl.BlockSpec((piece, cols), lambda n, j, idx: (0, n))
    return pl.pallas_call(
        functools.partial(out_kernel, last=last),
        grid_spec=pltpu.PrefetchScalarGridSpec(
            num_scalar_prefetch=1,
            grid=(d_model // cols, 4),
            in_specs=specs + [tile, tile] * last,
            out_specs=tile,
            scratch_shapes=[pltpu.VMEM((piece, cols), F32)] * last,
        ),
        out_shape=jax.ShapeDtypeStruct((piece, d_model), BF16 if last else F32),
        compiler_params=pltpu.CompilerParams(dimension_semantics=("arbitrary", "arbitrary"), vmem_limit_bytes=56 * 2**20),
        cost_estimate=pl.CostEstimate(flops=2 * piece * 4 * inner * d_model, bytes_accessed=6 * piece * d_model + 4 * inner * d_model * 2, transcendentals=0),
        name="out",
    )(idx, va, vb, w_all, *(extra or ()))


def head_tables(heads, inner, a_log, dt_bias, d_skip):
    hd = inner // heads
    reps = CH // heads
    zeros = jnp.zeros((6, CH), F32)
    dtp = jnp.concatenate([jnp.tile(dt_bias, reps)[None], jnp.tile(-jnp.exp(a_log) * LOG2E, reps)[None], zeros], axis=0)
    return dtp, jnp.repeat(d_skip, hd)[None]


def solution(mesh):
    n_sp = mesh.shape['sp']
    n_tp = mesh.shape['tp']
    n_dev = n_sp * n_tp
    far = n_tp // 2
    token_spec = P(('dp', 'sp', 'tp'), None)
    seg_spec = P(('dp', 'sp', 'tp'))
    weight_specs = (P(None, None, 'tp'), P(None, None, 'tp'), P(None, 'tp'), P(None, 'tp'), P(None, None, 'tp'), P('tp'), P(None, 'tp'), P('tp'), P('tp'), P('tp'), P('tp'), P('tp', None))
    ring = ('sp', 'tp')
    odd_even = lambda up, down, n: [(i, (i + (up if i % 2 else down)) % n) for i in range(n)]
    to_chip = odd_even(1, -1, n_dev)
    to_same = odd_even(-2, 2, n_dev)
    swap = odd_even(-1, 1, n_tp)
    hop = odd_even(-2, 2, n_tp)
    across = [(i, (i + far) % n_tp) for i in range(n_tp)]

    def body(x_loc, seg_loc, w_zx, w_bc, w_dt, conv_x, conv_bc, bias_x, bias_bc, a_log, dt_bias, d_skip, norm_w, w_out):
        piece, d_model = x_loc.shape
        inner = w_zx.shape[2]
        heads = w_dt.shape[1]
        hd = inner // heads
        ns = STATE_DIM
        width = inner + 2 * ns
        rows = math.gcd(piece, 512)
        sp = lax.axis_index('sp')
        tp = lax.axis_index('tp')
        dev = lax.axis_index(ring)
        even = dev % 2 == 0
        lane = jnp.arange(CH)[:, None]
        expm = ((lane < 3 * heads) & (lane % heads == jnp.arange(inner)[None, :] // hd)).astype(BF16)

        w_main = jnp.concatenate([w_zx[:, 1, :], w_bc.reshape(d_model, 2 * ns), jnp.tile(w_dt, (1, CH // heads))], axis=1)
        w_z = w_zx[:, 0, :]
        part = d_model // n_sp

        def gather(a, axis, tiled=True):
            return lax.all_gather(a, axis, axis=0, tiled=tiled)

        def project(a, w):
            return dotf(a, w).astype(BF16)

        mine = lax.dynamic_slice_in_dim(w_main, sp * part, part, axis=0)
        far_a = lax.ppermute(lax.ppermute(mine[:part // 2], 'tp', hop), 'tp', hop)
        far_b = lax.ppermute(lax.ppermute(mine[part // 2:], 'tp', hop), 'tp', hop)
        got_a = gather(far_a, 'sp', False)
        got_b = gather(far_b, 'sp', False)
        f_main = jnp.stack([got_a, got_b], axis=1).reshape(d_model, width + CH)

        x_par = lax.ppermute(x_loc, 'tp', swap)
        x_rec = lax.ppermute(x_loc, ring, to_chip)
        x_swp = lax.ppermute(x_rec, 'tp', swap)
        mine_z, _ = lax.optimization_barrier((lax.dynamic_slice_in_dim(w_z, sp * part, part, axis=0), x_rec))
        f_z = gather(lax.ppermute(lax.ppermute(mine_z, 'tp', hop), 'tp', hop), 'sp')
        out_part = w_out.shape[0] // n_sp
        w_part = lax.dynamic_slice_in_dim(w_out, sp * out_part, out_part, axis=0)
        w_all = gather(w_part, ('tp', 'sp'))

        pad = lambda v: jnp.pad(v, (0, width - v.shape[0]))[None]
        small = jnp.concatenate([
            jnp.concatenate([conv_x, conv_bc.reshape(CONV_WIDTH, 2 * ns)], axis=1).astype(F32),
            jnp.concatenate([bias_x, bias_bc.reshape(2 * ns)])[None].astype(F32),
            pad(norm_w.astype(F32)), pad(jnp.concatenate([a_log, dt_bias, d_skip])), jnp.zeros((1, width), F32)], axis=0)
        small_far = lax.ppermute(small, 'tp', across)

        def tables(t):
            cw = 0.5 * jnp.concatenate([t[:CONV_WIDTH + 1], jnp.zeros((3, width), F32)], axis=0)
            dtp, dskip = head_tables(heads, inner, t[6, :heads], t[6, heads:2 * heads], t[6, 2 * heads:3 * heads])
            return cw, dtp, dskip, t[5:6, :inner]

        tab = (tables(small), tables(small_far))

        seg_all = lax.all_gather(seg_loc, ring, axis=0, tiled=True)
        tails = lax.all_gather(x_loc[piece - 8:], ring, axis=0, tiled=True)
        seg_ext = jnp.concatenate([jnp.full((8,), seg_all[0] - 1, jnp.int32), seg_all])
        ids = (dev, dev + jnp.where(even, 1, -1), (dev + jnp.where(even, -1, 1)) % n_dev, (dev + jnp.where(even, 2, -2)) % n_dev)
        combs, comb_rows, tail_rows = [], [], []
        for pid in ids:
            win = lax.dynamic_slice_in_dim(seg_ext, pid * piece, piece + 8)
            rel = win[8:] - win[7]
            dist = sum((win[8 - j:8 - j + piece] == win[8:]).astype(jnp.int32) for j in (1, 2, 3))
            combs.append(jnp.broadcast_to((rel * 4 + dist)[:, None], (piece, CH)))
            comb_rows.append(rel.reshape(piece // CH, 1, CH))
            tail_rows.append(lax.dynamic_slice_in_dim(tails, ((pid + n_dev - 1) % n_dev) * 8, 8, axis=0))
        tail_rows = jnp.concatenate(tail_rows, axis=0)

        xs = (x_loc, x_par, x_rec, x_swp)
        w_mains = (w_main, f_main)
        scans = [[None, None], [None, None]]
        for shard, pair in ((0, 0), (0, 1), (1, 0), (1, 1)):
            cw, dtp, dskip, _ = tab[shard]
            halo = dotf(tail_rows, w_mains[shard][:, :width]).astype(BF16).reshape(4, 8, width)
            proj = [project(xs[2 * pair + k], w_mains[shard]) for k in range(2)]
            comb = jnp.concatenate(combs[2 * pair:2 * pair + 2], axis=0)
            comb_row = jnp.concatenate(comb_rows[2 * pair:2 * pair + 2], axis=0)
            scans[shard][pair] = ssd_call(proj, comb, comb_row, halo[2 * pair:2 * pair + 2], cw, dtp, dskip, expm, heads=heads, inner=inner, ns=ns, rows=rows)

        pick = lambda a, b: jnp.where(even, a, b)
        local, decs, runs = [], [], []
        for shard in range(2):
            end = [scans[shard][k // 2][3][k % 2] for k in range(4)]
            dec = [jnp.repeat(scans[shard][k // 2][4][k % 2, 0:1, :heads], hd, axis=1) for k in range(4)]
            order = lambda s: (pick(s[2], s[3]), pick(s[0], s[1]), pick(s[1], s[0]), pick(s[3], s[2]))
            e, q = order(end), order(dec)
            states, prods = [jnp.zeros_like(e[0])], [jnp.ones_like(q[0])]
            for k in range(4):
                states.append(q[k] * states[k] + e[k])
                prods.append(prods[k] * q[k])
            local.append(states)
            decs.append(prods)
            runs.append(jnp.concatenate([states[4], jnp.broadcast_to(prods[4], (8, inner))], axis=0))
        other = lax.ppermute(runs[1], 'tp', across)
        first = tp < far
        run_a = jnp.where(first, runs[0], other)
        run_b = jnp.where(first, other, runs[0])
        join = lambda p, q: jnp.concatenate([q[ns:ns + 1] * p[:ns] + q[:ns], q[ns:] * p[ns:]], axis=0)
        row = join(run_a, run_b)
        back = [lax.ppermute(row, 'sp', [(i, (i + k) % n_sp) for i in range(n_sp)]) for k in range(1, n_sp)] + [row]
        into = back[-1][:ns]
        for r in back[-2::-1]:
            into = r[ns:ns + 1] * into + r[:ns]
        into_b = run_a[ns:ns + 1] * into + run_a[:ns]
        into_mine = jnp.where(first, into, into_b)
        into_far = lax.ppermute(jnp.where(first, into_b, into), 'tp', across)

        w_zs = (w_z, f_z)
        zs = [[project(xs[k], w_zs[shard]) for k in range(4)] for shard in range(2)]
        vs = {}
        for k in (2, 3, 1, 0):
            sets = []
            for shard, came in ((0, into_mine), (1, into_far)):
                opts = ((1, 2), (2, 1), (0, 3), (3, 0))[k]
                st = pick(local[shard][opts[0]] + decs[shard][opts[0]] * came, local[shard][opts[1]] + decs[shard][opts[1]] * came).astype(BF16)
                y, c, corr, _, _ = scans[shard][k // 2]
                sets.append((y, c, corr, zs[shard][k], st, tab[shard][3]))
            vs[k] = gate_call(sets, expm, k % 2, piece, heads=heads, eps=NORM_EPS)
        v_far1 = lax.ppermute(vs[2], ring, to_chip)
        v_far2 = lax.ppermute(vs[3], ring, to_same)
        v_par = lax.ppermute(vs[1], 'tp', swap)
        shards_of = lambda g: [g % n_tp, (g + far) % n_tp]
        near = jnp.stack(shards_of(dev) + shards_of(ids[1])).astype(jnp.int32)
        away = jnp.stack(shards_of(ids[2]) + shards_of((dev + jnp.where(even, -2, 2)) % n_dev)).astype(jnp.int32)
        acc = out_call(near, vs[0], v_par, w_all, inner, None)
        return out_call(away, v_far1, v_far2, w_all, inner, (x_loc, acc))

    return jax.shard_map(body, mesh=mesh, in_specs=(token_spec, seg_spec) + weight_specs, out_specs=token_spec, check_vma=False)
```
